256 devices in a mesh: frame: 8 (over z_hi, x), tile: 32 (over y, z_lo, core).
Axes of the slice: x: 4, y: 4, z: 8 (z_hi: 2, z_lo: 4; z = z_hi * 4 + z_lo), core: 2. Of those that a mesh axis runs over, the one named last changes fastest.
Arguments:
- latents: bfloat16 [16, 128, 128, 512], P('frame', 'tile'), may hold values from -6 to 6
- conv_weight: bfloat16 [3, 3, 512, 512], replicated, may hold values from -0.09375 to 0.09375
- conv_bias: float32 [512], replicated, may hold values from -3 to 3
- query_weight: bfloat16 [512, 512], replicated, may hold values from -0.176776695 to 0.176776695
- key_weight: bfloat16 [512, 512], replicated, may hold values from -8 to 8
- value_weight: bfloat16 [512, 512], replicated, may hold values from -0.25 to 0.25
- out_weight: bfloat16 [512, 512], replicated, may hold values from -0.25 to 0.25
- cotangent: bfloat16 [16, 128, 128, 512], P('frame', 'tile'), may hold values from -0.01171875 to 0.01171875
Outputs:
- mixed_frames: bfloat16 [16, 128, 128, 512], P('frame', 'tile')
- conv_grad: float32 [512, 4608], P('tile', 'frame')
The draws below stay inside these ranges and needn't reach their ends.
All inputs are finite; a program needn't handle non-finite values.
Results may differ from the reference program's by a relative error of at most 0.0065.
Values may be sent and summed in bfloat16 or wider, within the bound.
No kernel may reach another device: no remote copies, remote signals or barrier semaphores. Data moves between devices by JAX's collectives and lax.ppermute only.
A program may use at most 128 MiB of HBM per device.

```python
import math
import jax
import jax.numpy as jnp
from jax import lax

C = 512
HEADS = 8
COLS = 128
FRAMES = 16
HEIGHT = 128


def shared_pair(key):
    base = jnp.clip(jax.random.normal(jax.random.fold_in(key, 11), (C, C), jnp.float32), -4.0, 4.0) / math.sqrt(C)
    other = jnp.clip(jax.random.normal(jax.random.fold_in(key, 12), (C, C), jnp.float32), -4.0, 4.0) / math.sqrt(C)
    return (base, other)


def draw_query_weight(key, part):
    base, other = shared_pair(key)
    return base.astype(jnp.bfloat16)


def draw_key_weight(key, part):
    base, other = shared_pair(key)
    result = other
    return result.astype(jnp.bfloat16)


def spiked(array, rng, source, target, blocks, factor):
    def block_of(position):
        return (jnp.arange(array.shape[position]) // (array.shape[position] // blocks)).reshape((-1,) + (1,) * (array.ndim - 1 - position))

    one_side = jax.random.permutation(rng, blocks)[block_of(target)]
    far = (block_of(target) + blocks // 2) % blocks
    return jnp.where((block_of(source) == one_side) | (block_of(source) == far), factor * array, array)


def level_of(rng, extent, shards, least, largest):
    def one(dim, shards_of):
        heights = jax.random.uniform(jax.random.fold_in(jax.random.fold_in(rng, 6), dim), (shards_of,), jnp.float32, least / len(shards), largest / len(shards))
        return jnp.repeat(jnp.exp(heights), extent[dim] // shards_of).reshape((-1,) + (1,) * (len(extent) - dim - 1))

    loudness = one(*shards[0])
    for cut in shards[1:]:
        loudness = loudness * one(*cut)
    return loudness


def centred(stream_key, extent, spread, most, shards=(), dtype=jnp.bfloat16):
    gain = level_of(stream_key, extent, shards, -0.22, 0.18) if shards else 1.0
    drawn = jax.random.normal(stream_key, extent, jnp.float32) * spread * gain
    return jnp.minimum(jnp.maximum(drawn, -most), most).astype(dtype)


def gaussian_with(key, extent, spread, reach, cuts, heavy, kind=jnp.bfloat16):
    drawn = spread * jax.random.normal(key, extent, jnp.float32)
    if cuts:
        drawn = drawn * level_of(key, extent, cuts, -0.22, 0.18)
    return jnp.clip(spiked(drawn, jax.random.fold_in(key, 3), *heavy), -reach, reach).astype(kind)


def setup_inputs(seed: int = 0) -> dict:
    key_list = jax.random.split(jax.random.key(seed), 9)
    latents = centred(key_list[0], (FRAMES, HEIGHT, COLS, C), 1.0, 6.0, ((0, 8), (1, 32)))
    conv_weight = centred(key_list[1], (3, 3, C, C), (9 * C) ** -0.5, 0.09375)
    conv_bias = centred(key_list[2], (C,), 0.5, 3.0, (), jnp.float32)
    query_weight = draw_query_weight(jax.random.fold_in(key_list[8], 71), 0)
    key_weight = draw_key_weight(jax.random.fold_in(key_list[8], 71), 0)
    value_weight = centred(key_list[5], (C, C), C ** -0.5, 0.25)
    out_weight = centred(key_list[6], (C, C), C ** -0.5, 0.25)
    cotangent = gaussian_with(key_list[7], (FRAMES, HEIGHT, COLS, C), ((FRAMES * HEIGHT * COLS) ** -0.5), 0.01171875, ((0, 8), (1, 32)), (1, 3, 32, 2.75))
    return dict(latents=latents, conv_weight=conv_weight, conv_bias=conv_bias, query_weight=query_weight, key_weight=key_weight, value_weight=value_weight, out_weight=out_weight, cotangent=cotangent)


def attention(hidden, query_weight, key_weight, value_weight, out_weight):
    frames, height, cols, channels = hidden.shape
    head_dim = channels // HEADS
    tokens = hidden.astype(jnp.float32).reshape(-1, channels)
    queries = jnp.dot(tokens, query_weight.astype(jnp.float32), precision=lax.Precision.HIGHEST).astype(jnp.bfloat16)
    key_rows = jnp.dot(tokens, key_weight.astype(jnp.float32), precision=lax.Precision.HIGHEST).astype(jnp.bfloat16)
    values = jnp.dot(tokens, value_weight.astype(jnp.float32), precision=lax.Precision.HIGHEST).astype(jnp.bfloat16)
    shaped = (frames, height * cols, HEADS, head_dim)
    queries = queries.astype(jnp.float32).reshape(shaped)
    key_rows = key_rows.astype(jnp.float32).reshape(shaped)
    values = values.astype(jnp.float32).reshape(shaped)
    scores = jnp.einsum('fphd,gphd->phfg', queries, key_rows, precision=lax.Precision.HIGHEST) / math.sqrt(head_dim)
    weights = jax.nn.softmax(scores, axis=-1).astype(jnp.bfloat16).astype(jnp.float32)
    head_out = jnp.einsum('phfg,gphd->fphd', weights, values, precision=lax.Precision.HIGHEST).astype(jnp.bfloat16)
    projected = jnp.dot(head_out.astype(jnp.float32).reshape(-1, channels), out_weight.astype(jnp.float32), precision=lax.Precision.HIGHEST)
    mixed = tokens + projected
    return mixed.astype(jnp.bfloat16).reshape(frames, height, cols, channels)

def reference(latents, conv_weight, conv_bias, query_weight, key_weight, value_weight, out_weight, cotangent):
    convolved = lax.conv_general_dilated(latents.astype(jnp.float32), conv_weight.astype(jnp.float32), (1, 1), ((1, 1), (1, 1)), dimension_numbers=('NHWC', 'HWIO', 'NHWC'), precision=lax.Precision.HIGHEST)
    hidden = jax.nn.silu(convolved + conv_bias).astype(jnp.bfloat16)
    mixed_frames = attention(hidden, query_weight, key_weight, value_weight, out_weight)
    frames, height, cols, channels = mixed_frames.shape
    padded = jnp.pad(mixed_frames.astype(jnp.float32), ((0, 0), (1, 1), (1, 1), (0, 0)))
    flat_cot = cotangent.astype(jnp.float32).reshape(-1, channels)
    pieces = []
    for row_shift in range(3):
        for col_shift in range(3):
            shifted = padded[:, row_shift:row_shift + height, col_shift:col_shift + cols, :].reshape(-1, channels)
            pieces.append(lax.dot_general(flat_cot, shifted, (((0,), (0,)), ((), ())), precision=lax.Precision.HIGHEST))
    conv_grad = jnp.concatenate(pieces, axis=1)
    return (mixed_frames, conv_grad)
```

```python
import math

import jax
import jax.numpy as jnp
from jax import lax
from jax.experimental import pallas as pl
from jax.experimental.pallas import tpu as pltpu
from jax.sharding import Mesh
from jax.sharding import PartitionSpec as P


HEADS = 8
FRAME = ("zh", "x")
TILE = ("y", "zl", "core")
F32 = jnp.float32
BF16 = jnp.bfloat16


def edge_rows(cells):
    count = math.prod(lax.axis_size(a) for a in TILE)
    head = cells[:, :1]
    tail = cells[:, -1:]
    above = lax.ppermute(tail, TILE, [(i, i + 1) for i in range(count - 1)])
    below = lax.ppermute(head, TILE, [(i + 1, i) for i in range(count - 1)])
    return above, below


def conv_kernel(above_ref, own_ref, below_ref, weight_ref, bias_ref, out_ref, rows_ref, acc_ref):
    s = pl.program_id(0)
    frames, height, cols, channels = own_ref.shape
    pixels = height * cols

    @pl.when(s == 0)
    def _():
        for f in range(frames):
            rows_ref[f, :cols] = above_ref[f, 0]
            rows_ref[f, cols : cols + pixels] = own_ref[f].reshape(pixels, channels)
            rows_ref[f, cols + pixels :] = below_ref[f, 0]

    column = lax.broadcasted_iota(jnp.int32, (pixels, 1), 0) % cols
    blocks = out_ref.shape[0]
    for f in range(frames):
        part = None
        for r in range(3):
            term = jnp.dot(
                rows_ref[f, r * cols : r * cols + pixels],
                weight_ref[r, 0],
                preferred_element_type=F32,
            )
            part = term if part is None else part + term

        @pl.when(s == 0)
        def _():
            acc_ref[f] = jnp.where(column > 0, pltpu.roll(part, 1, 0), 0.0)

        @pl.when(s == 1)
        def _():
            acc_ref[f] += part

        @pl.when(s == 2)
        def _():
            moved = jnp.where(column < cols - 1, pltpu.roll(part, pixels - 1, 0), 0.0)
            v = acc_ref[f] + moved + bias_ref[...]
            h = (v / (1.0 + jnp.exp(-v))).astype(BF16)
            h = h.reshape(height, blocks, cols // blocks, channels)
            for b in range(blocks):
                out_ref[b, f] = h[:, b]


def conv_silu(above, own, below, weight, bias, blocks):
    frames, height, cols, channels = own.shape
    edge = pl.BlockSpec(above.shape, lambda s: (0, 0, 0, 0))
    out_shape = (blocks, frames, height, cols // blocks, channels)
    return pl.pallas_call(
        conv_kernel,
        grid=(3,),
        in_specs=[
            edge,
            pl.BlockSpec(own.shape, lambda s: (0, 0, 0, 0)),
            edge,
            pl.BlockSpec((3, 1, channels, channels), lambda s: (0, s, 0, 0)),
            pl.BlockSpec((1, channels), lambda s: (0, 0)),
        ],
        out_specs=pl.BlockSpec(out_shape, lambda s: (0, 0, 0, 0, 0)),
        out_shape=jax.ShapeDtypeStruct(out_shape, BF16),
        scratch_shapes=[
            pltpu.VMEM((frames, (height + 2) * cols, channels), BF16),
            pltpu.VMEM((frames, height * cols, channels), F32),
        ],
        cost_estimate=pl.CostEstimate(flops=5 * 10**9, bytes_accessed=8 * 10**6, transcendentals=0),
        name="conv_silu",
    )(above, own, below, weight, bias.reshape(1, channels))


def attention_kernel(x_ref, wqkv_ref, wo_ref, out_ref):
    frames, _, cols, channels = x_ref.shape
    tokens = frames * cols
    x = x_ref[...].reshape(tokens, channels)
    qkv = jnp.dot(x, wqkv_ref[...], preferred_element_type=F32).astype(BF16)
    pair = 2 * (channels // HEADS)
    row = lax.broadcasted_iota(jnp.int32, (tokens, tokens), 0)
    col = lax.broadcasted_iota(jnp.int32, (tokens, tokens), 1)
    same = (row % cols) == (col % cols)
    lane = lax.broadcasted_iota(jnp.int32, (tokens, pair), 1)
    first = lane < pair // 2
    one = jnp.ones((tokens, pair), F32).astype(BF16)
    zero = jnp.zeros((tokens, pair), F32).astype(BF16)
    scale = math.log2(math.e) / math.sqrt(channels // HEADS)
    outs = []
    for p in range(HEADS // 2):
        lo = p * pair
        q = qkv[:, lo : lo + pair]
        k = qkv[:, channels + lo : channels + lo + pair]
        v = qkv[:, 2 * channels + lo : 2 * channels + lo + pair]
        total = None
        for half in range(2):
            keep = first if half == 0 else jnp.logical_not(first)
            k_half = jnp.where(keep, k, zero)
            s = lax.dot_general(q, k_half, (((1,), (1,)), ((), ())), preferred_element_type=F32)
            s = jnp.where(same, s, -1e30)
            m = jnp.max(s, axis=1, keepdims=True)
            e = jnp.exp2((s - m) * scale).astype(BF16)
            rhs = jnp.concatenate([jnp.where(keep, v, zero), jnp.where(keep, one, zero)], axis=1)
            part = jnp.dot(e, rhs, preferred_element_type=F32)
            total = part if total is None else total + part
        outs.append((total[:, :pair] / total[:, pair:]).astype(BF16))
    head_out = jnp.concatenate(outs, axis=1)
    mixed = x.astype(F32) + jnp.dot(head_out, wo_ref[...], preferred_element_type=F32)
    out_ref[...] = mixed.astype(BF16).reshape(out_ref.shape)


def attend(blocked, wqkv, wo):
    frames, rows, cols, channels = blocked.shape
    spec = pl.BlockSpec((frames, 1, cols, channels), lambda r: (0, r, 0, 0))
    return pl.pallas_call(
        attention_kernel,
        grid=(rows,),
        in_specs=[
            spec,
            pl.BlockSpec(wqkv.shape, lambda r: (0, 0)),
            pl.BlockSpec(wo.shape, lambda r: (0, 0)),
        ],
        out_specs=spec,
        out_shape=jax.ShapeDtypeStruct(blocked.shape, BF16),
        cost_estimate=pl.CostEstimate(flops=5 * 10**9, bytes_accessed=4 * 10**6, transcendentals=0),
        name="attend",
    )(blocked, wqkv, wo)


def grad_kernel(*refs):
    cots, mixes, out_ref = (refs[:3], refs[3:6]), refs[6:8], refs[8]
    r = pl.program_id(0)
    blocks, frames, height, width, channels = mixes[0].shape
    cols = blocks * width
    pixels = height * cols
    outs = cots[0][0].shape[0]
    acc = None
    for side in range(2):
        for f in range(frames):
            mix = jnp.concatenate(
                [mixes[side][b, f, y] for y in range(height) for b in range(blocks)], axis=0
            )
            start = pl.multiple_of(f * (pixels + 2 * cols) + (2 - r) * cols, cols)
            cot = jnp.concatenate([c[:, pl.ds(start, pixels)] for c in cots[side]], axis=0)
            part = jnp.dot(cot, mix, preferred_element_type=F32)
            acc = part if acc is None else acc + part
    flat = jnp.concatenate([acc[s * outs : (s + 1) * outs] for s in range(3)], axis=1).astype(BF16)
    places = out_ref.shape[0]
    block = channels * 9 // (2 * places)
    for step in range(3):

        @pl.when(r == step)
        def _():
            lo = step * 3 * channels
            for k in range(2 * places):
                a, b = max(lo, k * block), min(lo + 3 * channels, (k + 1) * block)
                if a < b:
                    to = (k // places) * block + a - k * block
                    out_ref[k % places, :, to : to + b - a] = flat[:, a - lo : b - lo]


def kernel_grad(cots, mixes, places):
    outs, width = cots[0].shape
    channels = mixes[0].shape[-1]
    out_shape = (places, outs, 9 * channels // places)
    cot_spec = pl.BlockSpec((outs, width), lambda r: (0, 0))
    mix_spec = pl.BlockSpec(mixes[0].shape, lambda r: (0, 0, 0, 0, 0))
    return pl.pallas_call(
        grad_kernel,
        grid=(3,),
        in_specs=[cot_spec] * 6 + [mix_spec] * 2,
        out_specs=pl.BlockSpec(out_shape, lambda r: (0, 0, 0)),
        out_shape=jax.ShapeDtypeStruct(out_shape, BF16),
        cost_estimate=pl.CostEstimate(flops=5 * 10**9, bytes_accessed=8 * 10**6, transcendentals=0),
        name="kernel_grad",
    )(*cots, *mixes)


def swap_core(value):
    return lax.ppermute(value, "core", [(0, 1), (1, 0)])


def shifted_cotangent(cotangent, above, below):
    rim = jnp.concatenate([above, cotangent, below], axis=1)
    _, _, cols, channels = rim.shape
    part = channels // 32
    core = lax.axis_index("core")
    source = lax.broadcasted_iota(jnp.int32, (channels, channels // 2), 0)
    target = lax.broadcasted_iota(jnp.int32, (channels, channels // 2), 1)
    wide = jnp.pad(rim, ((0, 0), (0, 0), (1, 1), (0, 0)))
    own, other = [], []
    for s in range(3):
        moved = wide[:, :, 2 - s : 2 - s + cols, :].reshape(-1, channels)
        for which, parts in ((core, own), (1 - core, other)):
            take = (source == (target // part) * 2 * part + which * part + target % part).astype(BF16)
            parts.append(
                lax.dot_general(take, moved, (((0,), (1,)), ((), ())), preferred_element_type=F32).astype(BF16)
            )
    return own + [swap_core(p) for p in other]


def sum_over_devices(partial):
    ny, nx, nzl, nzh = (lax.axis_size(a) for a in ("y", "x", "zl", "zh"))
    outs, width = partial.shape[1:]
    rows = outs // ny
    part = lax.all_to_all(partial.reshape(nx * ny, rows, width), ("x", "y"), 0, 0, tiled=True)
    part = jnp.sum(part.astype(F32), axis=0)
    part = part.reshape(nzl, rows // nzl, nzh, width // nzh).transpose(2, 0, 1, 3)
    part = part.reshape(nzh * nzl, rows // nzl, width // nzh)
    return jnp.sum(lax.all_to_all(part, ("zh", "zl"), 0, 0, tiled=True), axis=0)


def on_device(
    latents, conv_weight, conv_bias, query_weight, key_weight, value_weight, out_weight, cotangent
):
    above, below = edge_rows(latents)
    cot_above, cot_below = edge_rows(cotangent)
    count = math.prod(lax.axis_size(a) for a in FRAME)
    hidden = conv_silu(above, latents, below, conv_weight, conv_bias, count)
    blocked = lax.all_to_all(hidden, FRAME, 0, 0, tiled=True)
    cots = shifted_cotangent(cotangent, cot_above, cot_below)
    wqkv = jnp.concatenate([query_weight, key_weight, value_weight], axis=1)
    blocked, wqkv, *cots = lax.optimization_barrier((blocked, wqkv, *cots))
    pixel_mixed = attend(blocked.reshape(-1, *blocked.shape[2:]), wqkv, out_weight)
    sent = pixel_mixed.reshape(count, -1, *pixel_mixed.shape[1:])
    back = lax.all_to_all(sent, FRAME, 0, 0, tiled=True)
    mixed_frames = back.transpose(1, 2, 0, 3, 4).reshape(latents.shape)
    partial = kernel_grad(cots, (back, swap_core(back)), lax.axis_size("x"))
    return (mixed_frames, sum_over_devices(partial))


def solution(mesh):
    frame, tile = mesh.shape["frame"], mesh.shape["tile"]
    split = Mesh(
        mesh.devices.reshape(2, frame // 2, 4, tile // 8, 2), ("zh", "x", "y", "zl", "core")
    )
    in_specs = (
        P(FRAME, TILE, None, None),
        P(),
        P(),
        P(),
        P(),
        P(),
        P(),
        P(FRAME, TILE, None, None),
    )
    out_specs = (P(FRAME, TILE, None, None), P(TILE, FRAME))

    return jax.shard_map(
        on_device, mesh=split, in_specs=in_specs, out_specs=out_specs, check_vma=False
    )
```

```python
import math

import jax
import jax.numpy as jnp
from jax import lax
from jax.experimental import pallas as pl
from jax.experimental.pallas import tpu as pltpu
from jax.sharding import Mesh
from jax.sharding import PartitionSpec as P


HEADS = 8
FRAME = ("zh", "x")
TILE = ("y", "zl", "core")
F32 = jnp.float32
BF16 = jnp.bfloat16


def edge_rows(cells):
    count = math.prod(lax.axis_size(a) for a in TILE)
    head = cells[:, :1]
    tail = cells[:, -1:]
    above = lax.ppermute(tail, TILE, [(i, i + 1) for i in range(count - 1)])
    below = lax.ppermute(head, TILE, [(i + 1, i) for i in range(count - 1)])
    return above, below


def conv_kernel(above_ref, own_ref, below_ref, weight_ref, bias_ref, out_ref, rows_ref, acc_ref):
    s = pl.program_id(0)
    frames, height, cols, channels = own_ref.shape
    pixels = height * cols

    @pl.when(s == 0)
    def _():
        for f in range(frames):
            rows_ref[f, :cols] = above_ref[f, 0]
            rows_ref[f, cols : cols + pixels] = own_ref[f].reshape(pixels, channels)
            rows_ref[f, cols + pixels :] = below_ref[f, 0]

    column = lax.broadcasted_iota(jnp.int32, (pixels, 1), 0) % cols
    blocks = out_ref.shape[0]
    for f in range(frames):
        taps = [rows_ref[f, r * cols : r * cols + pixels] for r in range(3)]
        part = jnp.dot(
            jnp.concatenate(taps, axis=1),
            weight_ref[...].reshape(3 * channels, channels),
            preferred_element_type=F32,
        )

        @pl.when(s == 0)
        def _():
            acc_ref[f] = jnp.where(column > 0, pltpu.roll(part, 1, 0), 0.0)

        @pl.when(s == 1)
        def _():
            acc_ref[f] += part

        @pl.when(s == 2)
        def _():
            moved = jnp.where(column < cols - 1, pltpu.roll(part, pixels - 1, 0), 0.0)
            v = acc_ref[f] + moved + bias_ref[...]
            h = (v / (1.0 + jnp.exp(-v))).astype(BF16)
            h = h.reshape(height, blocks, cols // blocks, channels)
            for b in range(blocks):
                out_ref[b, f] = h[:, b]


def conv_silu(above, own, below, weight, bias, blocks):
    frames, height, cols, channels = own.shape
    edge = pl.BlockSpec(above.shape, lambda s: (0, 0, 0, 0))
    out_shape = (blocks, frames, height, cols // blocks, channels)
    return pl.pallas_call(
        conv_kernel,
        grid=(3,),
        in_specs=[
            edge,
            pl.BlockSpec(own.shape, lambda s: (0, 0, 0, 0)),
            edge,
            pl.BlockSpec((3, 1, channels, channels), lambda s: (0, s, 0, 0)),
            pl.BlockSpec((1, channels), lambda s: (0, 0)),
        ],
        out_specs=pl.BlockSpec(out_shape, lambda s: (0, 0, 0, 0, 0)),
        out_shape=jax.ShapeDtypeStruct(out_shape, BF16),
        scratch_shapes=[
            pltpu.VMEM((frames, (height + 2) * cols, channels), BF16),
            pltpu.VMEM((frames, height * cols, channels), F32),
        ],
        cost_estimate=pl.CostEstimate(flops=5 * 10**9, bytes_accessed=8 * 10**6, transcendentals=0),
        name="conv_silu",
    )(above, own, below, weight, bias.reshape(1, channels))


def attention_kernel(x_ref, wqkv_ref, wo_ref, out_ref):
    frames, _, cols, channels = x_ref.shape
    tokens = frames * cols
    x = x_ref[...].reshape(tokens, channels)
    qkv = jnp.dot(x, wqkv_ref[...], preferred_element_type=F32).astype(BF16)
    pair = 2 * (channels // HEADS)
    row = lax.broadcasted_iota(jnp.int32, (tokens, tokens), 0)
    col = lax.broadcasted_iota(jnp.int32, (tokens, tokens), 1)
    same = (row % cols) == (col % cols)
    lane = lax.broadcasted_iota(jnp.int32, (tokens, pair), 1)
    first = lane < pair // 2
    one = jnp.ones((tokens, pair), F32).astype(BF16)
    zero = jnp.zeros((tokens, pair), F32).astype(BF16)
    scale = math.log2(math.e) / math.sqrt(channels // HEADS)
    outs = []
    for p in range(HEADS // 2):
        lo = p * pair
        q = qkv[:, lo : lo + pair]
        k = qkv[:, channels + lo : channels + lo + pair]
        v = qkv[:, 2 * channels + lo : 2 * channels + lo + pair]
        total = None
        for half in range(2):
            keep = first if half == 0 else jnp.logical_not(first)
            k_half = jnp.where(keep, k, zero)
            s = lax.dot_general(q, k_half, (((1,), (1,)), ((), ())), preferred_element_type=F32)
            s = jnp.where(same, s, -1e30)
            m = jnp.max(s, axis=1, keepdims=True)
            e = jnp.exp2((s - m) * scale).astype(BF16)
            rhs = jnp.concatenate([jnp.where(keep, v, zero), jnp.where(keep, one, zero)], axis=1)
            part = jnp.dot(e, rhs, preferred_element_type=F32)
            total = part if total is None else total + part
        outs.append((total[:, :pair] / total[:, pair:]).astype(BF16))
    head_out = jnp.concatenate(outs, axis=1)
    mixed = x.astype(F32) + jnp.dot(head_out, wo_ref[...], preferred_element_type=F32)
    out_ref[...] = mixed.astype(BF16).reshape(out_ref.shape)


def attend(blocked, wqkv, wo):
    frames, rows, cols, channels = blocked.shape
    spec = pl.BlockSpec((frames, 1, cols, channels), lambda r: (0, r, 0, 0))
    return pl.pallas_call(
        attention_kernel,
        grid=(rows,),
        in_specs=[
            spec,
            pl.BlockSpec(wqkv.shape, lambda r: (0, 0)),
            pl.BlockSpec(wo.shape, lambda r: (0, 0)),
        ],
        out_specs=spec,
        out_shape=jax.ShapeDtypeStruct(blocked.shape, BF16),
        cost_estimate=pl.CostEstimate(flops=5 * 10**9, bytes_accessed=4 * 10**6, transcendentals=0),
        name="attend",
    )(blocked, wqkv, wo)


def grad_kernel(*refs):
    cots, mixes, out_ref = (refs[:3], refs[3:6]), refs[6:8], refs[8]
    blocks, frames, height, width, channels = mixes[0].shape
    cols = blocks * width
    pixels = height * cols
    outs = cots[0][0].shape[0]
    sides = [(side, f) for side in range(2) for f in range(frames)]
    mix = jnp.concatenate(
        [mixes[w][b, f, y] for w, f in sides for y in range(height) for b in range(blocks)], axis=0
    )
    places = out_ref.shape[0]
    block = channels * 9 // (2 * places)
    for r in range(3):
        lines = []
        for s in range(3):
            pieces = []
            for w, f in sides:
                start = f * (pixels + 2 * cols) + (2 - r) * cols
                pieces.append(cots[w][s][:, start : start + pixels])
            lines.append(jnp.concatenate(pieces, axis=1))
        acc = jnp.dot(jnp.concatenate(lines, axis=0), mix, preferred_element_type=F32)
        flat = [acc[s * outs : (s + 1) * outs] for s in range(3)]
        flat = jnp.concatenate(flat, axis=1).astype(BF16)
        lo = r * 3 * channels
        for k in range(2 * places):
            a, b = max(lo, k * block), min(lo + 3 * channels, (k + 1) * block)
            if a < b:
                to = (k // places) * block + a - k * block
                out_ref[k % places, :, to : to + b - a] = flat[:, a - lo : b - lo]


def kernel_grad(cots, mixes, places):
    outs, _ = cots[0].shape
    channels = mixes[0].shape[-1]
    out_shape = (places, outs, 9 * channels // places)
    whole = pl.BlockSpec(memory_space=pltpu.VMEM)
    return pl.pallas_call(
        grad_kernel,
        in_specs=[whole] * 8,
        out_specs=whole,
        out_shape=jax.ShapeDtypeStruct(out_shape, BF16),
        compiler_params=pltpu.CompilerParams(vmem_limit_bytes=40 * 2**20),
        cost_estimate=pl.CostEstimate(flops=5 * 10**9, bytes_accessed=8 * 10**6, transcendentals=0),
        name="kernel_grad",
    )(*cots, *mixes)


def swap_core(value):
    return lax.ppermute(value, "core", [(0, 1), (1, 0)])


def shifted_cotangent(cotangent, above, below):
    rim = jnp.concatenate([above, cotangent, below], axis=1)
    _, _, cols, channels = rim.shape
    part = channels // 32
    core = lax.axis_index("core")
    source = lax.broadcasted_iota(jnp.int32, (channels, channels // 2), 0)
    target = lax.broadcasted_iota(jnp.int32, (channels, channels // 2), 1)
    wide = jnp.pad(rim, ((0, 0), (0, 0), (1, 1), (0, 0)))
    own, other = [], []
    for s in range(3):
        moved = wide[:, :, 2 - s : 2 - s + cols, :].reshape(-1, channels)
        for which, parts in ((core, own), (1 - core, other)):
            take = (source == (target // part) * 2 * part + which * part + target % part).astype(BF16)
            parts.append(
                lax.dot_general(take, moved, (((0,), (1,)), ((), ())), preferred_element_type=F32).astype(BF16)
            )
    return own + [swap_core(p) for p in other]


def sum_over_devices(partial):
    ny, nx, nzl, nzh = (lax.axis_size(a) for a in ("y", "x", "zl", "zh"))
    outs, width = partial.shape[1:]
    rows = outs // ny
    part = lax.all_to_all(partial.reshape(nx * ny, rows, width), ("x", "y"), 0, 0, tiled=True)
    part = lax.optimization_barrier(jnp.sum(part.astype(F32), axis=0))
    part = part.reshape(nzl, rows // nzl, nzh, width // nzh).transpose(2, 0, 1, 3)
    part = part.reshape(nzh * nzl, rows // nzl, width // nzh).astype(BF16)
    part = lax.all_to_all(part, ("zh", "zl"), 0, 0, tiled=True)
    return jnp.sum(part.astype(F32), axis=0)


def on_device(
    latents, conv_weight, conv_bias, query_weight, key_weight, value_weight, out_weight, cotangent
):
    above, below = edge_rows(latents)
    cot_above, cot_below = edge_rows(cotangent)
    count = math.prod(lax.axis_size(a) for a in FRAME)
    hidden = conv_silu(above, latents, below, conv_weight, conv_bias, count)
    blocked = lax.all_to_all(hidden, FRAME, 0, 0, tiled=True)
    cots = shifted_cotangent(cotangent, cot_above, cot_below)
    wqkv = jnp.concatenate([query_weight, key_weight, value_weight], axis=1)
    blocked, wqkv, *cots = lax.optimization_barrier((blocked, wqkv, *cots))
    pixel_mixed = attend(blocked.reshape(-1, *blocked.shape[2:]), wqkv, out_weight)
    sent = pixel_mixed.reshape(count, -1, *pixel_mixed.shape[1:])
    back = lax.all_to_all(sent, FRAME, 0, 0, tiled=True)
    mixed_frames = back.transpose(1, 2, 0, 3, 4).reshape(latents.shape)
    partial = kernel_grad(cots, (back, swap_core(back)), lax.axis_size("x"))
    return (mixed_frames, sum_over_devices(partial))


def solution(mesh):
    frame, tile = mesh.shape["frame"], mesh.shape["tile"]
    split = Mesh(
        mesh.devices.reshape(2, frame // 2, 4, tile // 8, 2), ("zh", "x", "y", "zl", "core")
    )
    in_specs = (
        P(FRAME, TILE, None, None),
        P(),
        P(),
        P(),
        P(),
        P(),
        P(),
        P(FRAME, TILE, None, None),
    )
    out_specs = (P(FRAME, TILE, None, None), P(TILE, FRAME))

    return jax.shard_map(
        on_device, mesh=split, in_specs=in_specs, out_specs=out_specs, check_vma=False
    )
```

```python
import math

import jax
import jax.numpy as jnp
from jax import lax
from jax.experimental import pallas as pl
from jax.experimental.pallas import tpu as pltpu
from jax.sharding import Mesh
from jax.sharding import PartitionSpec as P


HEADS = 8
FRAME = ("zh", "x")
TILE = ("y", "zl", "core")
F32 = jnp.float32
BF16 = jnp.bfloat16


def edge_rows(cells):
    count = math.prod(lax.axis_size(a) for a in TILE)
    head = cells[:, :1]
    tail = cells[:, -1:]
    above = lax.ppermute(tail, TILE, [(i, i + 1) for i in range(count - 1)])
    below = lax.ppermute(head, TILE, [(i + 1, i) for i in range(count - 1)])
    return above, below


def conv_kernel(above_ref, own_ref, below_ref, weight_ref, bias_ref, out_ref, rows_ref, acc_ref):
    s = pl.program_id(0)
    frames, height, cols, channels = own_ref.shape
    pixels = height * cols

    @pl.when(s == 0)
    def _():
        for f in range(frames):
            rows_ref[f, :cols] = above_ref[f, 0]
            rows_ref[f, cols : cols + pixels] = own_ref[f].reshape(pixels, channels)
            rows_ref[f, cols + pixels :] = below_ref[f, 0]

    column = lax.broadcasted_iota(jnp.int32, (pixels, 1), 0) % cols
    blocks = out_ref.shape[0]
    for f in range(frames):
        taps = [rows_ref[f, r * cols : r * cols + pixels] for r in range(3)]
        part = jnp.dot(
            jnp.concatenate(taps, axis=1),
            weight_ref[...].reshape(3 * channels, channels),
            preferred_element_type=F32,
        )

        @pl.when(s == 0)
        def _():
            acc_ref[f] = jnp.where(column > 0, pltpu.roll(part, 1, 0), 0.0)

        @pl.when(s == 1)
        def _():
            acc_ref[f] += part

        @pl.when(s == 2)
        def _():
            moved = jnp.where(column < cols - 1, pltpu.roll(part, pixels - 1, 0), 0.0)
            v = acc_ref[f] + moved + bias_ref[...]
            h = (v / (1.0 + jnp.exp(-v))).astype(BF16)
            h = h.reshape(height, blocks, cols // blocks, channels)
            for b in range(blocks):
                out_ref[b, f] = h[:, b]


def conv_silu(above, own, below, weight, bias, blocks):
    frames, height, cols, channels = own.shape
    whole = pl.BlockSpec(memory_space=pltpu.VMEM)
    out_shape = (blocks, frames, height, cols // blocks, channels)
    return pl.pallas_call(
        conv_kernel,
        grid=(3,),
        in_specs=[
            whole,
            whole,
            whole,
            pl.BlockSpec((3, 1, channels, channels), lambda s: (0, s, 0, 0)),
            whole,
        ],
        out_specs=pl.BlockSpec(out_shape, lambda s: (0, 0, 0, 0, 0)),
        out_shape=jax.ShapeDtypeStruct(out_shape, BF16),
        scratch_shapes=[
            pltpu.VMEM((frames, (height + 2) * cols, channels), BF16),
            pltpu.VMEM((frames, height * cols, channels), F32),
        ],
        cost_estimate=pl.CostEstimate(flops=5 * 10**9, bytes_accessed=8 * 10**6, transcendentals=0),
        name="conv_silu",
    )(above, own, below, weight, bias.reshape(1, channels))


def attention_kernel(x_ref, wqkv_ref, wo_ref, out_ref):
    frames, _, cols, channels = x_ref.shape
    tokens = frames * cols
    x = x_ref[...].reshape(tokens, channels)
    qkv = jnp.dot(x, wqkv_ref[...], preferred_element_type=F32).astype(BF16)
    pair = 2 * (channels // HEADS)
    row = lax.broadcasted_iota(jnp.int32, (tokens, tokens), 0)
    col = lax.broadcasted_iota(jnp.int32, (tokens, tokens), 1)
    same = (row % cols) == (col % cols)
    lane = lax.broadcasted_iota(jnp.int32, (tokens, pair), 1)
    first = lane < pair // 2
    one = jnp.ones((tokens, pair), F32).astype(BF16)
    zero = jnp.zeros((tokens, pair), F32).astype(BF16)
    scale = math.log2(math.e) / math.sqrt(channels // HEADS)
    outs = []
    for p in range(HEADS // 2):
        lo = p * pair
        q = qkv[:, lo : lo + pair]
        k = qkv[:, channels + lo : channels + lo + pair]
        v = qkv[:, 2 * channels + lo : 2 * channels + lo + pair]
        total = None
        for half in range(2):
            keep = first if half == 0 else jnp.logical_not(first)
            k_half = jnp.where(keep, k, zero)
            s = lax.dot_general(q, k_half, (((1,), (1,)), ((), ())), preferred_element_type=F32)
            s = jnp.where(same, s, -1e30)
            m = jnp.max(s, axis=1, keepdims=True)
            e = jnp.exp2((s - m) * scale).astype(BF16)
            rhs = jnp.concatenate([jnp.where(keep, v, zero), jnp.where(keep, one, zero)], axis=1)
            part = jnp.dot(e, rhs, preferred_element_type=F32)
            total = part if total is None else total + part
        outs.append((total[:, :pair] / total[:, pair:]).astype(BF16))
    head_out = jnp.concatenate(outs, axis=1)
    mixed = x.astype(F32) + jnp.dot(head_out, wo_ref[...], preferred_element_type=F32)
    out_ref[...] = mixed.astype(BF16).reshape(out_ref.shape)


def attend(blocked, wqkv, wo):
    frames, rows, cols, channels = blocked.shape
    spec = pl.BlockSpec((frames, 1, cols, channels), lambda r: (0, r, 0, 0))
    return pl.pallas_call(
        attention_kernel,
        grid=(rows,),
        in_specs=[
            spec,
            pl.BlockSpec(memory_space=pltpu.VMEM),
            pl.BlockSpec(memory_space=pltpu.VMEM),
        ],
        out_specs=spec,
        out_shape=jax.ShapeDtypeStruct(blocked.shape, BF16),
        compiler_params=pltpu.CompilerParams(vmem_limit_bytes=24 * 2**20),
        cost_estimate=pl.CostEstimate(flops=5 * 10**9, bytes_accessed=4 * 10**6, transcendentals=0),
        name="attend",
    )(blocked, wqkv, wo)


def grad_kernel(*refs):
    cots, mixes, out_ref = (refs[:3], refs[3:6]), refs[6:8], refs[8]
    blocks, frames, height, width, channels = mixes[0].shape
    cols = blocks * width
    pixels = height * cols
    outs = cots[0][0].shape[0]
    sides = [(side, f) for side in range(2) for f in range(frames)]
    mix = jnp.concatenate(
        [mixes[w][b, f, y] for w, f in sides for y in range(height) for b in range(blocks)], axis=0
    )
    places = out_ref.shape[0]
    block = channels * 9 // (2 * places)
    for r in range(3):
        lines = []
        for s in range(3):
            pieces = []
            for w, f in sides:
                start = f * (pixels + 2 * cols) + (2 - r) * cols
                pieces.append(cots[w][s][:, start : start + pixels])
            lines.append(jnp.concatenate(pieces, axis=1))
        acc = jnp.dot(jnp.concatenate(lines, axis=0), mix, preferred_element_type=F32)
        flat = [acc[s * outs : (s + 1) * outs] for s in range(3)]
        flat = jnp.concatenate(flat, axis=1).astype(BF16)
        lo = r * 3 * channels
        for k in range(2 * places):
            a, b = max(lo, k * block), min(lo + 3 * channels, (k + 1) * block)
            if a < b:
                to = (k // places) * block + a - k * block
                out_ref[k % places, :, to : to + b - a] = flat[:, a - lo : b - lo]


def kernel_grad(cots, mixes, places):
    outs, _ = cots[0].shape
    channels = mixes[0].shape[-1]
    out_shape = (places, outs, 9 * channels // places)
    whole = pl.BlockSpec(memory_space=pltpu.VMEM)
    return pl.pallas_call(
        grad_kernel,
        in_specs=[whole] * 8,
        out_specs=whole,
        out_shape=jax.ShapeDtypeStruct(out_shape, BF16),
        compiler_params=pltpu.CompilerParams(vmem_limit_bytes=32 * 2**20),
        cost_estimate=pl.CostEstimate(flops=5 * 10**9, bytes_accessed=8 * 10**6, transcendentals=0),
        name="kernel_grad",
    )(*cots, *mixes)


def swap_core(value):
    return lax.ppermute(value, "core", [(0, 1), (1, 0)])


def shifted_cotangent(cotangent, above, below):
    rim = jnp.concatenate([above, cotangent, below], axis=1)
    _, _, cols, channels = rim.shape
    part = channels // 32
    core = lax.axis_index("core")
    source = lax.broadcasted_iota(jnp.int32, (channels, channels // 2), 0)
    target = lax.broadcasted_iota(jnp.int32, (channels, channels // 2), 1)
    wide = jnp.pad(rim, ((0, 0), (0, 0), (1, 1), (0, 0)))
    own, other = [], []
    for s in range(3):
        moved = wide[:, :, 2 - s : 2 - s + cols, :].reshape(-1, channels)
        for which, parts in ((core, own), (1 - core, other)):
            take = (source == (target // part) * 2 * part + which * part + target % part).astype(BF16)
            parts.append(
                lax.dot_general(take, moved, (((0,), (1,)), ((), ())), preferred_element_type=F32).astype(BF16)
            )
    return own + [swap_core(p) for p in other]


def sum_over_devices(partial):
    ny, nx, nzl, nzh = (lax.axis_size(a) for a in ("y", "x", "zl", "zh"))
    outs, width = partial.shape[1:]
    rows = outs // ny
    part = lax.all_to_all(partial.reshape(nx * ny, rows, width), ("x", "y"), 0, 0, tiled=True)
    part = lax.optimization_barrier(jnp.sum(part.astype(F32), axis=0))
    part = part.reshape(nzl, rows // nzl, nzh, width // nzh).transpose(2, 0, 1, 3)
    part = part.reshape(nzh * nzl, rows // nzl, width // nzh).astype(BF16)
    part = lax.all_to_all(part, ("zh", "zl"), 0, 0, tiled=True)
    return jnp.sum(part.astype(F32), axis=0)


def on_device(
    latents, conv_weight, conv_bias, query_weight, key_weight, value_weight, out_weight, cotangent
):
    above, below = edge_rows(latents)
    cot_above, cot_below = edge_rows(cotangent)
    count = math.prod(lax.axis_size(a) for a in FRAME)
    hidden = conv_silu(above, latents, below, conv_weight, conv_bias, count)
    blocked = lax.all_to_all(hidden, FRAME, 0, 0, tiled=True)
    cots = shifted_cotangent(cotangent, cot_above, cot_below)
    wqkv = jnp.concatenate([query_weight, key_weight, value_weight], axis=1)
    blocked, wqkv, *cots = lax.optimization_barrier((blocked, wqkv, *cots))
    pixel_mixed = attend(blocked.reshape(-1, *blocked.shape[2:]), wqkv, out_weight)
    sent = pixel_mixed.reshape(count, -1, *pixel_mixed.shape[1:])
    back = lax.all_to_all(sent, FRAME, 0, 0, tiled=True)
    mixed_frames = back.transpose(1, 2, 0, 3, 4).reshape(latents.shape)
    partial = kernel_grad(cots, (back, swap_core(back)), lax.axis_size("x"))
    return (mixed_frames, sum_over_devices(partial))


def solution(mesh):
    frame, tile = mesh.shape["frame"], mesh.shape["tile"]
    split = Mesh(
        mesh.devices.reshape(2, frame // 2, 4, tile // 8, 2), ("zh", "x", "y", "zl", "core")
    )
    in_specs = (
        P(FRAME, TILE, None, None),
        P(),
        P(),
        P(),
        P(),
        P(),
        P(),
        P(FRAME, TILE, None, None),
    )
    out_specs = (P(FRAME, TILE, None, None), P(TILE, FRAME))

    return jax.shard_map(
        on_device, mesh=split, in_specs=in_specs, out_specs=out_specs, check_vma=False
    )
```

```python
import math

import jax
import jax.numpy as jnp
from jax import lax
from jax.experimental import pallas as pl
from jax.experimental.pallas import tpu as pltpu
from jax.sharding import Mesh
from jax.sharding import PartitionSpec as P


HEADS = 8
FRAME = ("zh", "x")
TILE = ("y", "zl", "core")
F32 = jnp.float32
BF16 = jnp.bfloat16


def edge_rows(cells):
    count = math.prod(lax.axis_size(a) for a in TILE)
    head = cells[:, :1]
    tail = cells[:, -1:]
    above = lax.ppermute(tail, TILE, [(i, i + 1) for i in range(count - 1)])
    below = lax.ppermute(head, TILE, [(i + 1, i) for i in range(count - 1)])
    return above, below


def conv_kernel(
    above_ref, own_ref, below_ref, weight_ref, bias_ref, out_ref, taps_ref, held_ref, in_sem, out_sem
):
    loads = []
    for s in range(3):
        loads.append(pltpu.make_async_copy(weight_ref.at[:, s], taps_ref.at[s], in_sem.at[s]))
        loads[s].start()
    frames, height, cols, channels = own_ref.shape
    pixels = height * cols
    blocks = out_ref.shape[0]
    column = lax.broadcasted_iota(jnp.int32, (pixels, 1), 0) % cols
    stores = []
    for f in range(frames):
        rows = [above_ref[f, 0]] + [own_ref[f, y] for y in range(height)] + [below_ref[f, 0]]
        cells = [jnp.concatenate(rows[r : r + height], axis=0) for r in range(3)]
        cells = jnp.concatenate(cells, axis=1)
        parts = []
        for s in range(3):
            if f == 0:
                loads[s].wait()
            weight = taps_ref[s].reshape(3 * channels, channels)
            parts.append(jnp.dot(cells, weight, preferred_element_type=F32))
        left = jnp.where(column > 0, pltpu.roll(parts[0], 1, 0), 0.0)
        right = jnp.where(column < cols - 1, pltpu.roll(parts[2], pixels - 1, 0), 0.0)
        v = left + parts[1] + right + bias_ref[...]
        h = (v / (1.0 + jnp.exp(-v))).astype(BF16)
        h = h.reshape(height, blocks, cols // blocks, channels)
        for b in range(blocks):
            held_ref[f, b] = h[:, b]
        stores.append(pltpu.make_async_copy(held_ref.at[f], out_ref.at[:, f], out_sem.at[f]))
        stores[f].start()
    for store in stores:
        store.wait()


def conv_silu(above, own, below, weight, bias, blocks):
    frames, height, cols, channels = own.shape
    whole = pl.BlockSpec(memory_space=pltpu.VMEM)
    far = pl.BlockSpec(memory_space=pltpu.HBM)
    width = cols // blocks
    return pl.pallas_call(
        conv_kernel,
        in_specs=[whole, whole, whole, far, whole],
        out_specs=far,
        out_shape=jax.ShapeDtypeStruct((blocks, frames, height, width, channels), BF16),
        scratch_shapes=[
            pltpu.VMEM((3, 3, channels, channels), BF16),
            pltpu.VMEM((frames, blocks, height, width, channels), BF16),
            pltpu.SemaphoreType.DMA((3,)),
            pltpu.SemaphoreType.DMA((frames,)),
        ],
        cost_estimate=pl.CostEstimate(flops=5 * 10**9, bytes_accessed=8 * 10**6, transcendentals=0),
        name="conv_silu",
    )(above, own, below, weight, bias.reshape(1, channels))


def attention_kernel(x_ref, wqkv_ref, wo_ref, out_ref):
    frames, _, cols, channels = x_ref.shape
    tokens = frames * cols
    x = x_ref[...].reshape(tokens, channels)
    qkv = jnp.dot(x, wqkv_ref[...], preferred_element_type=F32).astype(BF16)
    pair = 2 * (channels // HEADS)
    row = lax.broadcasted_iota(jnp.int32, (tokens, tokens), 0)
    col = lax.broadcasted_iota(jnp.int32, (tokens, tokens), 1)
    same = (row % cols) == (col % cols)
    lane = lax.broadcasted_iota(jnp.int32, (tokens, pair), 1)
    first = lane < pair // 2
    one = jnp.ones((tokens, pair), F32).astype(BF16)
    zero = jnp.zeros((tokens, pair), F32).astype(BF16)
    scale = math.log2(math.e) / math.sqrt(channels // HEADS)
    outs = []
    for p in range(HEADS // 2):
        lo = p * pair
        q = qkv[:, lo : lo + pair]
        k = qkv[:, channels + lo : channels + lo + pair]
        v = qkv[:, 2 * channels + lo : 2 * channels + lo + pair]
        total = None
        for half in range(2):
            keep = first if half == 0 else jnp.logical_not(first)
            k_half = jnp.where(keep, k, zero)
            s = lax.dot_general(q, k_half, (((1,), (1,)), ((), ())), preferred_element_type=F32)
            s = jnp.where(same, s, -1e30)
            m = jnp.max(s, axis=1, keepdims=True)
            e = jnp.exp2((s - m) * scale).astype(BF16)
            rhs = jnp.concatenate([jnp.where(keep, v, zero), jnp.where(keep, one, zero)], axis=1)
            part = jnp.dot(e, rhs, preferred_element_type=F32)
            total = part if total is None else total + part
        outs.append((total[:, :pair] / total[:, pair:]).astype(BF16))
    head_out = jnp.concatenate(outs, axis=1)
    mixed = x.astype(F32) + jnp.dot(head_out, wo_ref[...], preferred_element_type=F32)
    out_ref[...] = mixed.astype(BF16).reshape(out_ref.shape)


def attend(blocked, wqkv, wo):
    frames, rows, cols, channels = blocked.shape
    spec = pl.BlockSpec((frames, 1, cols, channels), lambda r: (0, r, 0, 0))
    return pl.pallas_call(
        attention_kernel,
        grid=(rows,),
        in_specs=[
            spec,
            pl.BlockSpec(memory_space=pltpu.VMEM),
            pl.BlockSpec(memory_space=pltpu.VMEM),
        ],
        out_specs=spec,
        out_shape=jax.ShapeDtypeStruct(blocked.shape, BF16),
        compiler_params=pltpu.CompilerParams(vmem_limit_bytes=24 * 2**20),
        cost_estimate=pl.CostEstimate(flops=5 * 10**9, bytes_accessed=4 * 10**6, transcendentals=0),
        name="attend",
    )(blocked, wqkv, wo)


def grad_kernel(*refs):
    cots, mixes, out_ref = (refs[:3], refs[3:6]), refs[6:8], refs[8]
    blocks, frames, height, width, channels = mixes[0].shape
    cols = blocks * width
    pixels = height * cols
    outs = cots[0][0].shape[0]
    sides = [(side, f) for side in range(2) for f in range(frames)]
    mix = jnp.concatenate(
        [mixes[w][b, f, y] for w, f in sides for y in range(height) for b in range(blocks)], axis=0
    )
    places = out_ref.shape[0]
    block = channels * 9 // (2 * places)
    for r in range(3):
        lines = []
        for s in range(3):
            pieces = []
            for w, f in sides:
                start = f * (pixels + 2 * cols) + (2 - r) * cols
                pieces.append(cots[w][s][:, start : start + pixels])
            lines.append(jnp.concatenate(pieces, axis=1))
        acc = jnp.dot(jnp.concatenate(lines, axis=0), mix, preferred_element_type=F32)
        flat = [acc[s * outs : (s + 1) * outs] for s in range(3)]
        flat = jnp.concatenate(flat, axis=1).astype(BF16)
        lo = r * 3 * channels
        for k in range(2 * places):
            a, b = max(lo, k * block), min(lo + 3 * channels, (k + 1) * block)
            if a < b:
                to = (k // places) * block + a - k * block
                out_ref[k % places, :, to : to + b - a] = flat[:, a - lo : b - lo]


def kernel_grad(cots, mixes, places):
    outs, _ = cots[0].shape
    channels = mixes[0].shape[-1]
    out_shape = (places, outs, 9 * channels // places)
    whole = pl.BlockSpec(memory_space=pltpu.VMEM)
    return pl.pallas_call(
        grad_kernel,
        in_specs=[whole] * 8,
        out_specs=whole,
        out_shape=jax.ShapeDtypeStruct(out_shape, BF16),
        compiler_params=pltpu.CompilerParams(vmem_limit_bytes=32 * 2**20),
        cost_estimate=pl.CostEstimate(flops=5 * 10**9, bytes_accessed=8 * 10**6, transcendentals=0),
        name="kernel_grad",
    )(*cots, *mixes)


def swap_core(value):
    return lax.ppermute(value, "core", [(0, 1), (1, 0)])


def shifted_cotangent(cotangent, above, below):
    rim = jnp.concatenate([above, cotangent, below], axis=1)
    _, _, cols, channels = rim.shape
    part = channels // 32
    core = lax.axis_index("core")
    source = lax.broadcasted_iota(jnp.int32, (channels, channels // 2), 0)
    target = lax.broadcasted_iota(jnp.int32, (channels, channels // 2), 1)
    wide = jnp.pad(rim, ((0, 0), (0, 0), (1, 1), (0, 0)))
    own, other = [], []
    for s in range(3):
        moved = wide[:, :, 2 - s : 2 - s + cols, :].reshape(-1, channels)
        for which, parts in ((core, own), (1 - core, other)):
            take = (source == (target // part) * 2 * part + which * part + target % part).astype(BF16)
            parts.append(
                lax.dot_general(take, moved, (((0,), (1,)), ((), ())), preferred_element_type=F32).astype(BF16)
            )
    return own + [swap_core(p) for p in other]


def sum_over_devices(partial):
    ny, nx, nzl, nzh = (lax.axis_size(a) for a in ("y", "x", "zl", "zh"))
    outs, width = partial.shape[1:]
    rows = outs // ny
    part = lax.all_to_all(partial.reshape(nx * ny, rows, width), ("x", "y"), 0, 0, tiled=True)
    part = lax.optimization_barrier(jnp.sum(part.astype(F32), axis=0))
    part = part.reshape(nzl, rows // nzl, nzh, width // nzh).transpose(2, 0, 1, 3)
    part = part.reshape(nzh * nzl, rows // nzl, width // nzh).astype(BF16)
    part = lax.all_to_all(part, ("zh", "zl"), 0, 0, tiled=True)
    return jnp.sum(part.astype(F32), axis=0)


def on_device(
    latents, conv_weight, conv_bias, query_weight, key_weight, value_weight, out_weight, cotangent
):
    above, below = edge_rows(latents)
    cot_above, cot_below = edge_rows(cotangent)
    count = math.prod(lax.axis_size(a) for a in FRAME)
    hidden = conv_silu(above, latents, below, conv_weight, conv_bias, count)
    blocked = lax.all_to_all(hidden, FRAME, 0, 0, tiled=True)
    cots = shifted_cotangent(cotangent, cot_above, cot_below)
    wqkv = jnp.concatenate([query_weight, key_weight, value_weight], axis=1)
    blocked, wqkv, *cots = lax.optimization_barrier((blocked, wqkv, *cots))
    pixel_mixed = attend(blocked.reshape(-1, *blocked.shape[2:]), wqkv, out_weight)
    sent = pixel_mixed.reshape(count, -1, *pixel_mixed.shape[1:])
    back = lax.all_to_all(sent, FRAME, 0, 0, tiled=True)
    mixed_frames = back.transpose(1, 2, 0, 3, 4).reshape(latents.shape)
    partial = kernel_grad(cots, (back, swap_core(back)), lax.axis_size("x"))
    return (mixed_frames, sum_over_devices(partial))


def solution(mesh):
    frame, tile = mesh.shape["frame"], mesh.shape["tile"]
    split = Mesh(
        mesh.devices.reshape(2, frame // 2, 4, tile // 8, 2), ("zh", "x", "y", "zl", "core")
    )
    in_specs = (
        P(FRAME, TILE, None, None),
        P(),
        P(),
        P(),
        P(),
        P(),
        P(),
        P(FRAME, TILE, None, None),
    )
    out_specs = (P(FRAME, TILE, None, None), P(TILE, FRAME))

    return jax.shard_map(
        on_device, mesh=split, in_specs=in_specs, out_specs=out_specs, check_vma=False
    )
```
